32 devices in a mesh: dp: 4 (over y, x), mp: 8 (over z, core).
Axes of the slice: x: 2, y: 2, z: 4, core: 2. Of those that a mesh axis runs over, the one named last changes fastest.
Arguments:
- grad_out: bfloat16 [4096, 2560], P(('dp', 'mp')), may hold values from -0.5 to 0.5
- hidden_act: bfloat16 [4096, 13824], P('dp', 'mp'), may hold values from -6 to 6
- carried: bfloat16 [4, 13824, 2560], P('dp', 'mp'), may hold values from -6 to 6
- prior_right: float32 [2560, 64], replicated, may hold values from -6 to 6
Outputs:
- residual_out: bfloat16 [4, 13824, 2560], P('dp', 'mp')
- next_right: float32 [2560, 64], replicated
The draws below stay inside these ranges and needn't reach their ends.
All inputs are finite; a program needn't handle non-finite values.
Results may differ from the reference program's by a relative error of at most 0.0058.
Values may be sent and summed in bfloat16 or wider, within the bound.
A program may use at most 128 MiB of HBM per device.

```python
import jax
import jax.numpy as jnp
from jax import lax

D = 2560
FF = 13824
RANK = 64
TOK_DEV = 1024
TOKENS = 4096
N_DP = 4


def steps_of(rng, extent, cuts, least, top_value):
    factor_of = 1.0
    for dim, parts in cuts:
        heights = jax.random.uniform(jax.random.fold_in(jax.random.fold_in(rng, 6), dim), (parts,), jnp.float32, least / len(cuts), top_value / len(cuts))
        factor_of = factor_of * jnp.repeat(jnp.exp(heights), extent[dim] // parts).reshape((-1,) + (1,) * (len(extent) - 1 - dim))
    return factor_of


def noise(key, extent, scale, most, cuts=(), kind=jnp.bfloat16):
    loudness = steps_of(key, extent, cuts, -0.22, 0.18) if cuts else 1.0
    array = jax.random.normal(key, extent, jnp.float32) * scale * loudness
    return jnp.minimum(jnp.maximum(array, -most), most).astype(kind)


def setup_inputs(seed: int = 0) -> dict:
    arg_keys = jax.random.split(jax.random.key(seed), 5)
    grad_out = noise(arg_keys[0], (TOKENS, D), (TOK_DEV ** -0.5), 0.5, ((0, 32),))
    hidden_act = noise(arg_keys[1], (TOKENS, FF), 1.0, 6.0, ((0, 4), (1, 8)))
    carried = noise(arg_keys[2], (N_DP, FF, D), 1.0, 6.0, ((0, 4), (1, 8)))
    prior_right = noise(arg_keys[3], (D, RANK), 1.0, 6.0, (), jnp.float32)
    return dict(grad_out=grad_out, hidden_act=hidden_act, carried=carried, prior_right=prior_right)


highest = lax.Precision.HIGHEST
over_rows = (((0,), (0,)), ((), ()))

def ortho_from(gram_matrix, left_rows):
    rank_size = gram_matrix.shape[0]
    identity = jnp.eye(rank_size, dtype=jnp.float32)
    ridge_shift = 0.001 * jnp.trace(gram_matrix) / rank_size
    cholesky_factor = jnp.linalg.cholesky(gram_matrix + ridge_shift * identity)
    inverse = lax.linalg.triangular_solve(cholesky_factor, identity, left_side=True, lower=True)
    return jnp.dot(left_rows.astype(jnp.float32), inverse.T.astype(jnp.float32), precision=highest, preferred_element_type=jnp.float32)

def reference(grad_out, hidden_act, carried, prior_right):

    def merged_of(replica):
        offset = (replica * TOK_DEV).astype(jnp.int32)
        act_rows = lax.dynamic_slice_in_dim(hidden_act, offset, TOK_DEV, 0)
        out_rows = lax.dynamic_slice_in_dim(grad_out, offset, TOK_DEV, 0)
        weight_grad = lax.dot_general(act_rows.astype(jnp.float32), out_rows.astype(jnp.float32), over_rows, preferred_element_type=jnp.float32)
        own = lax.dynamic_index_in_dim(carried, replica, 0, keepdims=False)
        return own.astype(jnp.float32) + weight_grad

    def accumulate(running, replica):
        return (running + merged_of(replica), None)
    replicas = jnp.arange(N_DP, dtype=jnp.int32)
    summed, _ = lax.scan(accumulate, jnp.zeros((FF, D), jnp.float32), replicas)
    left_whole = jnp.dot(summed.astype(jnp.float32), prior_right.astype(jnp.float32), precision=highest, preferred_element_type=jnp.float32)
    gram_matrix = jnp.dot(left_whole.T.astype(jnp.float32), left_whole.astype(jnp.float32), precision=highest, preferred_element_type=jnp.float32)
    ortho_left = ortho_from(gram_matrix, left_whole)
    next_right = lax.dot_general(summed.astype(jnp.float32), ortho_left.astype(jnp.float32), over_rows, precision=highest, preferred_element_type=jnp.float32) / N_DP
    low_rank = jnp.dot(ortho_left.astype(jnp.float32), next_right.T.astype(jnp.float32), precision=highest, preferred_element_type=jnp.float32)
    residual_out = lax.map(lambda replica: (merged_of(replica) - low_rank).astype(jnp.bfloat16), replicas)
    return (residual_out, next_right)
```

```python
import functools

import jax
import jax.numpy as jnp
from jax import lax
from jax.experimental import pallas as pl
from jax.experimental.pallas import tpu as pltpu
from jax.sharding import PartitionSpec as P

highest = lax.Precision.HIGHEST
over_rows = (((0,), (0,)), ((), ()))
F32, BF16 = jnp.float32, jnp.bfloat16


def lane_tiles(extent, step):
    return [(s, min(step, extent - s)) for s in range(0, extent, step)]


def split2(x, axis):
    hi = x.astype(BF16)
    lo = (x - hi.astype(F32)).astype(BF16)
    return jnp.concatenate([hi, lo], axis=axis)


def halves(x, rank):
    return x[:, :rank] + x[:, rank:]


def inverse_factor(gram):
    n = gram.shape[0]
    ri = lax.broadcasted_iota(jnp.int32, (n, 2 * n), 0)
    ci = lax.broadcasted_iota(jnp.int32, (n, 2 * n), 1)
    eye = (ri == ci)[:, :n]
    trace = jnp.sum(jnp.sum(jnp.where(eye, gram, 0.0), axis=1, keepdims=True), axis=0, keepdims=True)
    ridged = gram + jnp.where(eye, 0.001 * (trace / n), 0.0)
    start = jnp.concatenate([ridged, jnp.where(eye, 1.0, 0.0)], axis=1)

    def step(k, a):
        row = jnp.sum(jnp.where(ri == k, a, 0.0), axis=0, keepdims=True)
        col = jnp.sum(jnp.where(ci == k, a, 0.0), axis=1, keepdims=True)
        piv = jnp.sum(jnp.where(ci[:1] == k, row, 0.0), axis=1, keepdims=True)
        r = 1.0 / jnp.sqrt(piv)
        scaled = row * r
        return jnp.where(ri == k, scaled, jnp.where(ri > k, a - (col * r) * scaled, a))

    return lax.fori_loop(0, n, step, start)[:, n:]


def fused_kernel(dp, mp, g_hbm, h_hbm, c_hbm, p_ref, merged_hbm, l2_ref, a2_ref, nr_ref,
                 h_v, c_v, m_v, gall, p2, pj, x_v, lbuf, l_v, gbuf, racc, rsend, rrecv,
                 dbuf, abuf, local_sem, out_sem, pj_s, pj_r, g_s, g_r, l_s, l_r,
                 gr_s, gr_r, rs_s, rs_r, d_s, d_r, a_s, a_r):
    tok, dim = g_hbm.shape
    rank = p_ref.shape[1]
    ff = c_hbm.shape[0]
    half = ff // 2
    me_d, me_m = lax.axis_index("dp"), lax.axis_index("mp")

    def push(src_of, dst, size, axis, me, send, recv):
        copies = []
        for k in range(1, size):
            peer = lax.rem(me + k, size)
            copies.append(pltpu.make_async_remote_copy(
                src_ref=src_of(peer), dst_ref=dst.at[me], send_sem=send.at[k],
                recv_sem=recv.at[me], device_id={axis: peer},
                device_id_type=pl.DeviceIdType.MESH))
            copies[-1].start()
        return copies

    def arrive(dst, size, axis, me, send, recv):
        for k in range(1, size):
            peer = lax.rem(me + k, size)
            pltpu.make_async_remote_copy(
                src_ref=dst.at[peer], dst_ref=dst.at[peer], send_sem=send.at[k],
                recv_sem=recv.at[peer], device_id={axis: peer},
                device_id_type=pl.DeviceIdType.MESH).wait_recv()

    own = pltpu.make_async_copy(g_hbm, gall.at[me_m], local_sem.at[0])
    own.start()
    load_c = pltpu.make_async_copy(c_hbm, c_v, local_sem.at[1])
    load_c.start()
    load_h = pltpu.make_async_copy(h_hbm, h_v, local_sem.at[2])
    load_h.start()

    barrier = pltpu.get_barrier_semaphore()
    for k in range(1, mp):
        pl.semaphore_signal(barrier, inc=1, device_id={"mp": lax.rem(me_m + k, mp)},
                            device_id_type=pl.DeviceIdType.MESH)
    for k in range(1, dp):
        pl.semaphore_signal(barrier, inc=1, device_id={"dp": lax.rem(me_d + k, dp)},
                            device_id_type=pl.DeviceIdType.MESH)

    p2[...] = split2(p_ref[...], 1)
    own.wait()
    proj = halves(jnp.dot(gall[me_m], p2[...], preferred_element_type=F32), rank)
    pj[me_m] = split2(proj, 1)
    pl.semaphore_wait(barrier, mp + dp - 2)

    sent = push(lambda peer: pj.at[me_m], pj, mp, "mp", me_m, pj_s, pj_r)
    sent += push(lambda peer: g_hbm, gall, mp, "mp", me_m, g_s, g_r)

    load_c.wait()
    for s in (0, half):
        x_v[s:s + half, :] = jnp.dot(c_v[s:s + half, :], p2[...], preferred_element_type=F32)
    load_h.wait()
    arrive(pj, mp, "mp", me_m, pj_s, pj_r)
    pj_all = pj[...].reshape(mp * tok, 2 * rank)
    for s, w in lane_tiles(ff, 256):
        x_v[s:s + w, :] += lax.dot_general(h_v[:, s:s + w], pj_all, over_rows,
                                           preferred_element_type=F32)
    lbuf[me_d] = jnp.concatenate(
        [halves(x_v[:half, :], rank), halves(x_v[half:, :], rank)], axis=1).astype(BF16)
    sent += push(lambda peer: lbuf.at[me_d], lbuf, dp, "dp", me_d, l_s, l_r)
    arrive(lbuf, dp, "dp", me_d, l_s, l_r)
    packed = lbuf[0].astype(F32)
    for k in range(1, dp):
        packed = packed + lbuf[k].astype(F32)
    packed = packed.astype(BF16)
    l_v[:half, :] = packed[:, :rank]
    l_v[half:, :] = packed[:, rank:]
    l2_ref[...] = jnp.concatenate([l_v[...], l_v[...]], axis=1)
    gram = lax.dot_general(l_v[...], l_v[...], over_rows, preferred_element_type=F32)
    gbuf[me_m] = jnp.concatenate([gram, gram], axis=1)
    sent += push(lambda peer: gbuf.at[me_m], gbuf, mp, "mp", me_m, gr_s, gr_r)

    arrive(gall, mp, "mp", me_m, g_s, g_r)
    racc[...] = jnp.zeros_like(racc)
    outs = []
    for t, (s, w) in enumerate(lane_tiles(ff, 256)):
        @pl.loop(0, dim // 512)
        def _(n, s=s, w=w):
            cols = pl.ds(pl.multiple_of(n * 512, 512), 512)
            tile = c_v[s:s + w, cols].astype(F32) + lax.dot_general(
                h_v[:, s:s + w], gall[:, :, cols].reshape(mp * tok, 512), over_rows,
                preferred_element_type=F32)
            m_v[s:s + w, cols] = tile
            racc[:, cols] += lax.dot_general(l_v[s:s + w, :], tile.astype(BF16), over_rows,
                                             preferred_element_type=F32)
        outs.append(pltpu.make_async_copy(
            m_v.at[pl.ds(s, w)], merged_hbm.at[pl.ds(s, w)], out_sem.at[t]))
        outs[-1].start()

    part = rank // mp
    for j in range(mp):
        rsend[j] = racc[j * part:(j + 1) * part, :]
    sent += push(lambda peer: rsend.at[peer], rrecv, mp, "mp", me_m, rs_s, rs_r)

    arrive(gbuf, mp, "mp", me_m, gr_s, gr_r)
    gram = gbuf[0]
    for j in range(1, mp):
        gram = gram + gbuf[j]
    inverse = inverse_factor(gram[:, :rank])

    arrive(rrecv, mp, "mp", me_m, rs_s, rs_r)
    acc = rsend[me_m]
    for k in range(1, mp):
        acc = acc + rrecv[lax.rem(me_m + k, mp)]
    dbuf[me_d] = acc
    sent += push(lambda peer: dbuf.at[me_d], dbuf, dp, "dp", me_d, d_s, d_r)
    arrive(dbuf, dp, "dp", me_d, d_s, d_r)
    acc = dbuf[0]
    for k in range(1, dp):
        acc = acc + dbuf[k]
    abuf[me_m] = acc
    sent += push(lambda peer: abuf.at[me_m], abuf, mp, "mp", me_m, a_s, a_r)
    arrive(abuf, mp, "mp", me_m, a_s, a_r)
    for j in range(mp):
        racc[j * part:(j + 1) * part, :] = abuf[j]
    right = jnp.dot(inverse, racc[...], precision=highest, preferred_element_type=F32) / dp
    nr_ref[...] = right
    coef = lax.dot_general(inverse, right, over_rows, precision=highest,
                           preferred_element_type=F32)
    a2_ref[...] = split2(coef, 0)
    for c in sent:
        c.wait_send()
    for c in outs:
        c.wait()


def per_device(dp, mp, grad_out, hidden_act, carried, prior_right):
    tok, dim = grad_out.shape
    rank = prior_right.shape[1]
    ff = hidden_act.shape[1]
    toks = hidden_act.shape[0]
    part = rank // mp
    dma = pltpu.SemaphoreType.DMA
    anywhere = pl.BlockSpec(memory_space=pl.ANY)
    vmem = pl.BlockSpec(memory_space=pltpu.VMEM)
    merged, left2, coef2, right_t = pl.pallas_call(
        functools.partial(fused_kernel, dp, mp),
        out_shape=(
            jax.ShapeDtypeStruct((ff, dim), F32),
            jax.ShapeDtypeStruct((ff, 2 * rank), BF16),
            jax.ShapeDtypeStruct((2 * rank, dim), BF16),
            jax.ShapeDtypeStruct((rank, dim), F32),
        ),
        in_specs=[anywhere, anywhere, anywhere, vmem],
        out_specs=(anywhere, vmem, vmem, vmem),
        scratch_shapes=[
            pltpu.VMEM((toks, ff), BF16),
            pltpu.VMEM((ff, dim), BF16),
            pltpu.VMEM((ff, dim), F32),
            pltpu.VMEM((mp, tok, dim), BF16),
            pltpu.VMEM((dim, 2 * rank), BF16),
            pltpu.VMEM((mp, tok, 2 * rank), BF16),
            pltpu.VMEM((ff, 2 * rank), F32),
            pltpu.VMEM((dp, ff // 2, 2 * rank), BF16),
            pltpu.VMEM((ff, rank), BF16),
            pltpu.VMEM((mp, rank, 2 * rank), F32),
            pltpu.VMEM((rank, dim), F32),
            pltpu.VMEM((mp, part, dim), F32),
            pltpu.VMEM((mp, part, dim), F32),
            pltpu.VMEM((dp, part, dim), F32),
            pltpu.VMEM((mp, part, dim), F32),
            dma((3,)),
            dma((len(lane_tiles(ff, 256)),)),
            dma((mp,)), dma((mp,)), dma((mp,)), dma((mp,)),
            dma((dp,)), dma((dp,)),
            dma((mp,)), dma((mp,)), dma((mp,)), dma((mp,)),
            dma((dp,)), dma((dp,)), dma((mp,)), dma((mp,)),
        ],
        compiler_params=pltpu.CompilerParams(
            collective_id=0, has_side_effects=True, vmem_limit_bytes=62 * 1024 * 1024),
    )(grad_out, hidden_act, carried[0], prior_right)
    low_rank = jnp.dot(left2, coef2, preferred_element_type=F32)
    residual_out = (merged - low_rank).astype(BF16)[None]
    return (residual_out, right_t.T)


def solution(mesh):
    in_specs = (P(("dp", "mp"), None), P("dp", "mp"), P("dp", "mp", None), P())
    out_specs = (P("dp", "mp", None), P())
    return jax.shard_map(
        functools.partial(per_device, mesh.shape["dp"], mesh.shape["mp"]),
        mesh=mesh, in_specs=in_specs, out_specs=out_specs, check_vma=False
    )
```

```python
import functools

import jax
import jax.numpy as jnp
from jax import lax
from jax.experimental import pallas as pl
from jax.experimental.pallas import tpu as pltpu
from jax.sharding import PartitionSpec as P

highest = lax.Precision.HIGHEST
over_rows = (((0,), (0,)), ((), ()))
F32, BF16 = jnp.float32, jnp.bfloat16


def lane_tiles(extent, step):
    return [(s, min(step, extent - s)) for s in range(0, extent, step)]


def split2(x, axis):
    hi = x.astype(BF16)
    lo = (x - hi.astype(F32)).astype(BF16)
    return jnp.concatenate([hi, lo], axis=axis)


def halves(x, rank):
    return x[:, :rank] + x[:, rank:]


def inverse_factor(gram):
    n = gram.shape[0]
    ri = lax.broadcasted_iota(jnp.int32, (n, 2 * n), 0)
    ci = lax.broadcasted_iota(jnp.int32, (n, 2 * n), 1)
    eye = (ri == ci)[:, :n]
    trace = jnp.sum(jnp.sum(jnp.where(eye, gram, 0.0), axis=1, keepdims=True), axis=0, keepdims=True)
    ridged = gram + jnp.where(eye, 0.001 * (trace / n), 0.0)
    start = jnp.concatenate([ridged, jnp.where(eye, 1.0, 0.0)], axis=1)

    def step(k, a):
        row = jnp.sum(jnp.where(ri == k, a, 0.0), axis=0, keepdims=True)
        col = jnp.sum(jnp.where(ci == k, a, 0.0), axis=1, keepdims=True)
        piv = jnp.sum(jnp.where(ci[:1] == k, row, 0.0), axis=1, keepdims=True)
        r = 1.0 / jnp.sqrt(piv)
        scaled = row * r
        return jnp.where(ri == k, scaled, jnp.where(ri > k, a - (col * r) * scaled, a))

    return lax.fori_loop(0, n, step, start)[:, n:]


def fused_kernel(dp, mp, g_hbm, h_hbm, c_hbm, p_ref, merged_hbm, l2_ref, a2_ref, nr_ref,
                 h_v, c_v, m_v, gall, p2, pj, x_v, lbuf, l_v, gbuf, racc, rsend, rpair, rsum, rrecv,
                 dbuf, abuf, local_sem, out_sem, pj_s, pj_r, g_s, g_r, l_s, l_r,
                 gr_s, gr_r, rs_s, rs_r, pair_r, d_s, d_r, a_s, a_r):
    tok, dim = g_hbm.shape
    rank = p_ref.shape[0]
    ff = c_hbm.shape[0]
    half = ff // 2
    me_d, me_m = lax.axis_index("dp"), lax.axis_index("mp")

    def push(src_of, dst, size, axis, me, send, recv):
        copies = []
        for k in range(1, size):
            peer = lax.rem(me + k, size)
            copies.append(pltpu.make_async_remote_copy(
                src_ref=src_of(peer), dst_ref=dst.at[me], send_sem=send.at[k],
                recv_sem=recv.at[me], device_id={axis: peer},
                device_id_type=pl.DeviceIdType.MESH))
            copies[-1].start()
        return copies

    def arrive(dst, size, axis, me, send, recv):
        for k in range(1, size):
            peer = lax.rem(me + k, size)
            pltpu.make_async_remote_copy(
                src_ref=dst.at[peer], dst_ref=dst.at[peer], send_sem=send.at[k],
                recv_sem=recv.at[peer], device_id={axis: peer},
                device_id_type=pl.DeviceIdType.MESH).wait_recv()

    core = lax.rem(me_m, 2)
    me_z = me_m // 2
    partner = me_m + 1 - 2 * core
    chips = mp // 2

    def to_mp(src, dst, send, recv, peer):
        return pltpu.make_async_remote_copy(
            src_ref=src, dst_ref=dst, send_sem=send, recv_sem=recv,
            device_id={"mp": peer}, device_id_type=pl.DeviceIdType.MESH)

    def gather_start(src, buf, send, recv):
        copies = []
        for k in range(1, chips):
            copies.append(to_mp(src, buf.at[me_m], send.at[k], recv.at[me_m],
                                lax.rem(me_m + 2 * k, mp)))
        copies.append(to_mp(src, buf.at[me_m], send.at[0], recv.at[me_m], partner))
        for c in copies:
            c.start()
        return copies

    def gather_finish(buf, send, recv):
        copies = []
        for step in range(1, chips):
            k = (step + 1) // 2 if step % 2 else chips - step // 2
            block = lax.rem(me_m + 2 * k, mp)
            to_mp(buf.at[block], buf.at[block], send.at[chips + k], recv.at[block],
                  partner).wait_recv()
            copies.append(to_mp(buf.at[block], buf.at[block], send.at[chips + k],
                                recv.at[block], partner))
            copies[-1].start()
        for k in range(chips):
            block = lax.rem(partner + 2 * k, mp)
            to_mp(buf.at[block], buf.at[block], send.at[0], recv.at[block],
                  partner).wait_recv()
        return copies

    own = pltpu.make_async_copy(g_hbm, gall.at[me_m], local_sem.at[0])
    own.start()
    load_c = pltpu.make_async_copy(c_hbm, c_v, local_sem.at[1])
    load_c.start()
    load_h = pltpu.make_async_copy(h_hbm, h_v, local_sem.at[2])
    load_h.start()

    barrier = pltpu.get_barrier_semaphore()
    for k in range(1, mp):
        pl.semaphore_signal(barrier, inc=1, device_id={"mp": lax.rem(me_m + k, mp)},
                            device_id_type=pl.DeviceIdType.MESH)
    for k in range(1, dp):
        pl.semaphore_signal(barrier, inc=1, device_id={"dp": lax.rem(me_d + k, dp)},
                            device_id_type=pl.DeviceIdType.MESH)

    p2[...] = split2(p_ref[...].T, 1)
    own.wait()
    proj = halves(jnp.dot(gall[me_m], p2[...], preferred_element_type=F32), rank)
    pj[me_m] = split2(proj, 1)
    pl.semaphore_wait(barrier, mp + dp - 2)

    sent = gather_start(pj.at[me_m], pj, pj_s, pj_r)
    sent += gather_start(g_hbm, gall, g_s, g_r)

    load_c.wait()
    for s in (0, half):
        x_v[s:s + half, :] = jnp.dot(c_v[s:s + half, :], p2[...], preferred_element_type=F32)
    load_h.wait()
    sent += gather_finish(pj, pj_s, pj_r)
    pj_all = pj[...].reshape(mp * tok, 2 * rank)
    for s, w in lane_tiles(ff, 256):
        x_v[s:s + w, :] += jnp.dot(h_v[s:s + w, :], pj_all, preferred_element_type=F32)
    lbuf[me_d] = jnp.concatenate(
        [halves(x_v[:half, :], rank), halves(x_v[half:, :], rank)], axis=1).astype(BF16)
    sent += push(lambda peer: lbuf.at[me_d], lbuf, dp, "dp", me_d, l_s, l_r)
    arrive(lbuf, dp, "dp", me_d, l_s, l_r)
    packed = lbuf[0].astype(F32)
    for k in range(1, dp):
        packed = packed + lbuf[k].astype(F32)
    packed = packed.astype(BF16)
    l_v[:half, :] = packed[:, :rank]
    l_v[half:, :] = packed[:, rank:]
    l2_ref[...] = jnp.concatenate([l_v[...], l_v[...]], axis=1)
    gram = lax.dot_general(l_v[...], l_v[...], over_rows, preferred_element_type=F32)
    gbuf[me_m] = jnp.concatenate([gram, gram], axis=1)
    sent += gather_start(gbuf.at[me_m], gbuf, gr_s, gr_r)

    sent += gather_finish(gall, g_s, g_r)
    racc[...] = jnp.zeros_like(racc)
    outs = []
    for t, (s, w) in enumerate(lane_tiles(ff, 256)):
        @pl.loop(0, dim // 512)
        def _(n, s=s, w=w):
            cols = pl.ds(pl.multiple_of(n * 512, 512), 512)
            tile = c_v[s:s + w, cols].astype(F32) + jnp.dot(
                h_v[s:s + w, :], gall[:, :, cols].reshape(mp * tok, 512),
                preferred_element_type=F32)
            m_v[s:s + w, cols] = tile
            racc[:, cols] += lax.dot_general(l_v[s:s + w, :], tile.astype(BF16), over_rows,
                                             preferred_element_type=F32)
        outs.append(pltpu.make_async_copy(
            m_v.at[pl.ds(s, w)], merged_hbm.at[pl.ds(s, w)], out_sem.at[t]))
        outs[-1].start()

    part = rank // mp
    for j in range(mp):
        rsend[j % 2, j // 2] = racc[j * part:(j + 1) * part, :]
    pair = to_mp(rsend.at[1 - core], rpair, rs_s.at[0], pair_r, partner)
    pair.start()
    sent += gather_finish(gbuf, gr_s, gr_r)
    pair.wait()
    for z in range(chips):
        rsum[z] = rsend[core, z] + rpair[z]
    for k in range(1, chips):
        z = lax.rem(me_z + k, chips)
        c = to_mp(rsum.at[z], rrecv.at[me_z], rs_s.at[k], rs_r.at[me_z], 2 * z + core)
        c.start()
        sent.append(c)
    gram = gbuf[0]
    for j in range(1, mp):
        gram = gram + gbuf[j]
    inverse = inverse_factor(gram[:, :rank])

    acc = rsum[me_z]
    for k in range(1, chips):
        z = lax.rem(me_z + k, chips)
        to_mp(rrecv.at[z], rrecv.at[z], rs_s.at[k], rs_r.at[z], 2 * z + core).wait_recv()
        acc = acc + rrecv[z]
    dbuf[me_d] = acc
    sent += push(lambda peer: dbuf.at[me_d], dbuf, dp, "dp", me_d, d_s, d_r)
    arrive(dbuf, dp, "dp", me_d, d_s, d_r)
    acc = dbuf[0]
    for k in range(1, dp):
        acc = acc + dbuf[k]
    abuf[me_m] = acc
    sent += gather_start(abuf.at[me_m], abuf, a_s, a_r)
    sent += gather_finish(abuf, a_s, a_r)
    for j in range(mp):
        racc[j * part:(j + 1) * part, :] = abuf[j]
    right = jnp.dot(inverse, racc[...], precision=highest, preferred_element_type=F32) / dp
    nr_ref[...] = right
    coef = lax.dot_general(inverse, right, over_rows, precision=highest,
                           preferred_element_type=F32)
    a2_ref[...] = split2(coef, 0)
    for c in sent:
        c.wait_send()
    for c in outs:
        c.wait()


def per_device(dp, mp, grad_out, hidden_act, carried, prior_right):
    tok, dim = grad_out.shape
    rank = prior_right.shape[1]
    ff = hidden_act.shape[1]
    toks = hidden_act.shape[0]
    part = rank // mp
    dma = pltpu.SemaphoreType.DMA
    anywhere = pl.BlockSpec(memory_space=pl.ANY)
    vmem = pl.BlockSpec(memory_space=pltpu.VMEM)
    merged, left2, coef2, right_t = pl.pallas_call(
        functools.partial(fused_kernel, dp, mp),
        out_shape=(
            jax.ShapeDtypeStruct((ff, dim), F32),
            jax.ShapeDtypeStruct((ff, 2 * rank), BF16),
            jax.ShapeDtypeStruct((2 * rank, dim), BF16),
            jax.ShapeDtypeStruct((rank, dim), F32),
        ),
        in_specs=[anywhere, anywhere, anywhere, vmem],
        out_specs=(anywhere, vmem, vmem, vmem),
        scratch_shapes=[
            pltpu.VMEM((ff, toks), BF16),
            pltpu.VMEM((ff, dim), BF16),
            pltpu.VMEM((ff, dim), F32),
            pltpu.VMEM((mp, tok, dim), BF16),
            pltpu.VMEM((dim, 2 * rank), BF16),
            pltpu.VMEM((mp, tok, 2 * rank), BF16),
            pltpu.VMEM((ff, 2 * rank), F32),
            pltpu.VMEM((dp, ff // 2, 2 * rank), BF16),
            pltpu.VMEM((ff, rank), BF16),
            pltpu.VMEM((mp, rank, 2 * rank), F32),
            pltpu.VMEM((rank, dim), F32),
            pltpu.VMEM((2, mp // 2, part, dim), F32),
            pltpu.VMEM((mp // 2, part, dim), F32),
            pltpu.VMEM((mp // 2, part, dim), F32),
            pltpu.VMEM((mp // 2, part, dim), F32),
            pltpu.VMEM((dp, part, dim), F32),
            pltpu.VMEM((mp, part, dim), F32),
            dma((3,)),
            dma((len(lane_tiles(ff, 256)),)),
            dma((mp,)), dma((mp,)), dma((mp,)), dma((mp,)),
            dma((dp,)), dma((dp,)),
            dma((mp,)), dma((mp,)), dma((mp // 2,)), dma((mp // 2,)), dma,
            dma((dp,)), dma((dp,)), dma((mp,)), dma((mp,)),
        ],
        compiler_params=pltpu.CompilerParams(
            collective_id=0, has_side_effects=True, vmem_limit_bytes=62 * 1024 * 1024),
    )(grad_out, hidden_act.T, carried[0], prior_right.T)
    low_rank = jnp.dot(left2, coef2, preferred_element_type=F32)
    residual_out = (merged - low_rank).astype(BF16)[None]
    return (residual_out, right_t.T)


def solution(mesh):
    in_specs = (P(("dp", "mp"), None), P("dp", "mp"), P("dp", "mp", None), P())
    out_specs = (P("dp", "mp", None), P())
    return jax.shard_map(
        functools.partial(per_device, mesh.shape["dp"], mesh.shape["mp"]),
        mesh=mesh, in_specs=in_specs, out_specs=out_specs, check_vma=False
    )
```
